32 devices in a mesh: grp: 8 (over y, x, core), cube: 4 (over z).
Axes of the slice: x: 2, y: 2, z: 4, core: 2. Of those that a mesh axis runs over, the one named last changes fastest.
Arguments:
- params: float32 [8, 4, 4096, 128], P('grp', 'cube'), may hold values from -8 to 8
- estimate: float32 [8, 4, 4096, 128], P('grp', 'cube'), may hold values from -6 to 6
- neighbour_sum: float32 [8, 4, 4096, 128], P('grp', 'cube'), may hold values from -10 to 10
- gradient: bfloat16 [8, 4, 4096, 128], P('grp', 'cube'), may hold values from -6 to 6
- block_ids: int32 [8, 4, 128], P('grp', 'cube'), may hold values from 0 to 4095, as said below
Outputs:
- new_params: float32 [8, 4, 4096, 128], P('grp', 'cube')
- new_estimate: float32 [8, 4, 4096, 128], P('grp', 'cube')
- new_neighbour_sum: float32 [8, 4, 4096, 128], P('grp', 'cube')
- consensus: float32 [1], replicated
The draws below stay inside these ranges and needn't reach their ends.
Inputs may be any that keep to these rules, and one draw needn't show every extreme that they name: `block_ids`: each replica's row holds 128 distinct block numbers in ascending order.
All inputs are finite; a program needn't handle non-finite values.
Results may differ from the reference program's by a relative error of at most 0.003.
Values may be sent and summed in bfloat16 or wider, within the bound.
A program may use at most 64 MiB of HBM per device.

```python
import jax
import jax.numpy as jnp
import numpy as np
from jax import lax

BLOCK = 128
NB = 4096
KEPT = 128
CUBE_BITS = 2
GROUP_BITS = 3
N_GRP = 8
N_CUBE = 4


def draw_params(key, part):
    extent = (N_GRP, N_CUBE, NB, BLOCK)
    replicas = N_GRP * N_CUBE
    position = jnp.arange(replicas, dtype=jnp.float32).reshape(N_GRP, N_CUBE, 1, 1) / (replicas - 1)
    values = jax.random.normal(key, extent, jnp.float32) * (0.5 * 3.0 ** position)
    return jnp.clip(values, -8.0, 8.0)


def draw_block_ids(key, part):
    keys = jax.random.split(key, N_GRP * N_CUBE)

    def one_replica(replica_key):
        return jnp.sort(jax.random.permutation(replica_key, NB)[:KEPT])
    return jax.vmap(one_replica)(keys).reshape(N_GRP, N_CUBE, KEPT).astype(jnp.int32)


def shard_levels(own_key, dims, pieces, smallest, high):
    factor_of, own = 1.0, jax.random.fold_in(own_key, 6)
    for axis_at, blocks in pieces:
        heights = jnp.exp(jax.random.uniform(jax.random.fold_in(own, axis_at), (blocks,), jnp.float32, smallest / len(pieces), high / len(pieces)))
        factor_of = factor_of * jnp.repeat(heights, dims[axis_at] // blocks).reshape([-1 if axis == axis_at else 1 for axis in range(len(dims))])
    return factor_of


def centred(stream_key, shape, scale, reach, pieces=(), kind=jnp.bfloat16):
    values = jax.random.normal(stream_key, shape, jnp.float32) * scale
    if len(pieces) > 0:
        values = shard_levels(stream_key, shape, pieces, -0.22, 0.18) * values
    return jnp.clip(values, min=-reach, max=reach).astype(kind)


def setup_inputs(seed: int = 0) -> dict:
    streams_of = jax.random.split(jax.random.key(seed), 6)
    params = draw_params(jax.random.fold_in(streams_of[5], 71), 0)
    estimate = centred(streams_of[1], (N_GRP, N_CUBE, NB, BLOCK), 1.0, 6.0, ((0, 8), (1, 4)), jnp.float32)
    neighbour_sum = centred(streams_of[2], (N_GRP, N_CUBE, NB, BLOCK), 1.7, 10.0, ((0, 8), (1, 4)), jnp.float32)
    gradient = centred(streams_of[3], (N_GRP, N_CUBE, NB, BLOCK), 1.0, 6.0, ((0, 8), (1, 4)))
    block_ids = draw_block_ids(jax.random.fold_in(streams_of[5], 71), 0)
    return {"params": params, "estimate": estimate, "neighbour_sum": neighbour_sum, "gradient": gradient, "block_ids": block_ids}


LEARN_RATE = 0.1
INNER_RATE = 0.6
OUTER_RATE = 0.5

def take_rows(table, chosen):
    return table[chosen]

def add_rows(target, chosen, values):
    return target.at[chosen].add(values.astype(jnp.float32))

def reference(params, estimate, neighbour_sum, gradient, block_ids):
    groups = N_GRP
    cubes = N_CUBE
    gather_all = jax.vmap(jax.vmap(take_rows))
    scatter_all = jax.vmap(jax.vmap(add_rows))
    stepped = params - LEARN_RATE * gradient.astype(jnp.float32)
    picked = (gather_all(stepped, block_ids) - gather_all(estimate, block_ids)).astype(jnp.bfloat16)
    new_estimate = scatter_all(estimate, block_ids, picked)
    summed = neighbour_sum
    for level in range(CUBE_BITS):
        partner = np.arange(cubes) ^ 1 << level
        summed = scatter_all(summed, block_ids[:, partner], picked[:, partner])
    mixed = stepped + INNER_RATE * (summed - CUBE_BITS * new_estimate) / (CUBE_BITS + 1)
    group_mean = lax.optimization_barrier(jnp.sum(mixed, axis=1)) / cubes
    combined = group_mean
    for level in range(GROUP_BITS):
        partner = np.arange(groups) ^ 1 << level
        combined = combined + group_mean[partner]
    shortfall = combined / (GROUP_BITS + 1) - group_mean
    new_params = mixed + OUTER_RATE * shortfall[:, None]
    consensus = jnp.sqrt(jnp.sum(shortfall * shortfall) / (groups * NB * BLOCK)).reshape(1)
    return (new_params, new_estimate, summed, consensus)
```

```python
import functools

import jax
import jax.numpy as jnp
from jax import lax
from jax.experimental import pallas as pl
from jax.experimental.pallas import tpu as pltpu
from jax.sharding import PartitionSpec as P

LEARN_RATE = 0.1
INNER_RATE = 0.6
OUTER_RATE = 0.5
CHUNK = 256
ENDS = 6
HOP = 2
SWAP = 2
BACK = 2
PIECES = 4

MESH = pl.DeviceIdType.MESH
F32, BF16 = jnp.float32, jnp.bfloat16


def kernel(
    n_cube, n_grp,
    params, estimate, neighbour_sum, gradient, ids,
    p_v, e_v, n_v, consensus,
    g_v, picked, theirs, their_ids,
    from_left, from_right, outgoing, mean_out, mean_in, fix, shortfall_v,
    spread, spread_grp, spread_cube,
    load_sem, pick_send, pick_recv, id_send, id_recv,
    up_send, left_recv, right_recv, mean_send, mean_recv,
    fix_send, fix_recv,
    sg_send, sg_recv, sc_send, sc_recv,
):
    me, grp = lax.axis_index("cube"), lax.axis_index("grp")
    rows, width = p_v.shape
    kept = picked.shape[0]
    chunks = rows // CHUNK
    cube_bits, grp_bits = n_cube.bit_length() - 1, n_grp.bit_length() - 1
    piece = rows // PIECES

    def load(which, at):
        src, dst = ((params, p_v), (gradient, g_v), (estimate, e_v), (neighbour_sum, n_v))[which]
        window = pl.ds(at * piece, piece)
        return pltpu.make_async_copy(src.at[window], dst.at[window], load_sem.at[which, at])

    for at in range(PIECES):
        for which in range(3):
            load(which, at).start()
    for at in range(PIECES):
        load(3, at).start()

    barrier = pltpu.get_barrier_semaphore()
    for d in range(1, n_cube):
        pl.semaphore_signal(barrier, inc=1, device_id={"cube": (me + d) % n_cube}, device_id_type=MESH)
    for d in range(1, n_grp):
        pl.semaphore_signal(barrier, inc=1, device_id={"grp": (grp + d) % n_grp}, device_id_type=MESH)
    pl.semaphore_wait(barrier, n_cube + n_grp - 2)

    def flip(index, level):
        bit = 1 << level
        return index + bit - 2 * bit * ((index // bit) % 2)

    def copy(src, dst, send, recv, **device):
        return pltpu.make_async_remote_copy(
            src_ref=src, dst_ref=dst, send_sem=send, recv_sem=recv, device_id=device, device_id_type=MESH
        )

    def id_copy(level):
        return copy(ids, their_ids.at[level], id_send.at[level], id_recv.at[level], cube=flip(me, level))

    def pick_copy(level):
        return copy(
            picked, theirs.at[pl.ds(level * kept, kept)], pick_send.at[level], pick_recv.at[level],
            cube=flip(me, level),
        )

    for level in range(cube_bits):
        id_copy(level).start()

    square = (kept, kept)
    own_ids = ids[...]
    diagonal = lax.broadcasted_iota(jnp.int32, square, 0) == lax.broadcasted_iota(jnp.int32, square, 1)
    id_column = jnp.sum(jnp.where(diagonal, jnp.broadcast_to(own_ids, square), 0), axis=1, keepdims=True)

    def pick(j, total):
        window = pl.ds(pl.multiple_of(j * CHUNK, CHUNK), CHUNK)
        stepped = p_v[window, :] - LEARN_RATE * g_v[window, :].astype(F32)
        p_v[window, :] = stepped
        change = (stepped - e_v[window, :]).astype(BF16)
        row = lax.broadcasted_iota(jnp.int32, (kept, CHUNK), 1) + j * CHUNK
        hot = (row == id_column).astype(F32).astype(BF16)
        return total + jnp.dot(hot, change, preferred_element_type=F32)

    total = jnp.zeros((kept, width), F32)
    for at in range(PIECES):
        for which in range(3):
            load(which, at).wait()
        each = piece // CHUNK
        total = lax.fori_loop(at * each, (at + 1) * each, pick, total)
    picked[...] = total.astype(BF16)
    for level in range(cube_bits):
        pick_copy(level).start()
    for at in range(PIECES):
        load(3, at).wait()
    spread[...] = jnp.zeros_like(spread)
    for level in range(cube_bits):
        id_copy(level).wait()
    for level in range(cube_bits):
        pick_copy(level).wait()

    def window_of(j):
        return pl.ds(pl.multiple_of(j * CHUNK, CHUNK), CHUNK)

    def mix(j):
        window = window_of(j)
        row = lax.broadcasted_iota(jnp.int32, (CHUNK, kept), 0) + j * CHUNK

        def hot(names):
            return (row == names).astype(F32).astype(BF16)

        e = e_v[window, :] + jnp.dot(hot(own_ids), picked[...], preferred_element_type=F32)
        marks = jnp.concatenate([hot(their_ids[level]) for level in range(cube_bits)], axis=1)
        s = n_v[window, :] + jnp.dot(marks, theirs[...], preferred_element_type=F32)
        e_v[window, :] = e
        n_v[window, :] = s
        p_v[window, :] = p_v[window, :] + (INNER_RATE / (cube_bits + 1)) * (s - cube_bits * e)

    low, high = n_cube // 2 - 1, n_cube // 2
    owners = sorted({0, n_cube - 1, low, high})

    def owner(j):
        return jnp.where(j < ENDS, (j % 2) * (n_cube - 1), low + j % 2)

    def valid(j):
        return jnp.logical_and(j >= 0, j < chunks)

    def right_copy(j):
        return copy(outgoing.at[j], from_left.at[j], up_send.at[j], left_recv.at[j], cube=me + 1)

    def left_copy(j):
        return copy(outgoing.at[j], from_right.at[j], up_send.at[j], right_recv.at[j], cube=me - 1)

    def wait_left(j):
        copy(from_left.at[j], from_left.at[j], up_send.at[j], left_recv.at[j], cube=me).wait_recv()

    def wait_right(j):
        copy(from_right.at[j], from_right.at[j], up_send.at[j], right_recv.at[j], cube=me).wait_recv()

    def mean_copy(level, j):
        return copy(
            mean_out.at[j], mean_in.at[level, j], mean_send.at[level, j], mean_recv.at[level, j],
            grp=flip(grp, level),
        )

    def fix_copy(side, j):
        return copy(fix.at[j], fix.at[j], fix_send.at[side, j], fix_recv.at[j], cube=me + (1 if side else -1))

    def finish(j, amount):
        p_v[window_of(j), :] = p_v[window_of(j), :] + OUTER_RATE * amount

    def spread_copy_grp(d):
        return copy(
            spread, spread_grp.at[grp], sg_send.at[d], sg_recv.at[grp], grp=(grp + d) % n_grp
        )

    def spread_copy_cube(d):
        return copy(
            spread_grp.at[n_grp], spread_cube.at[me], sc_send.at[d], sc_recv.at[me], cube=(me + d) % n_cube
        )

    def climb(step):
        j = step - me * HOP

        @pl.when(valid(j))
        def _():
            @pl.when(me < owner(j))
            def _():
                @pl.when(me > 0)
                def _():
                    wait_left(j)
                    outgoing[j] = (p_v[window_of(j), :] + from_left[j].astype(F32)).astype(BF16)

                @pl.when(me == 0)
                def _():
                    outgoing[j] = p_v[window_of(j), :].astype(BF16)

                right_copy(j).start()

        i = step - (n_cube - 1 - me) * HOP

        @pl.when(valid(i))
        def _():
            @pl.when(me > owner(i))
            def _():
                @pl.when(me < n_cube - 1)
                def _():
                    wait_right(i)
                    outgoing[i] = (p_v[window_of(i), :] + from_right[i].astype(F32)).astype(BF16)

                @pl.when(me == n_cube - 1)
                def _():
                    outgoing[i] = p_v[window_of(i), :].astype(BF16)

                left_copy(i).start()

    def reach(at):
        return max(at, n_cube - 1 - at) * HOP

    my_reach = jnp.where(2 * me < n_cube, n_cube - 1 - me, me) * HOP

    def own(step):
        j = step - my_reach

        @pl.when(valid(j))
        def _():
            @pl.when(me == owner(j))
            def _():
                shortfall_v[j] = p_v[window_of(j), :]

                @pl.when(me > 0)
                def _():
                    wait_left(j)
                    shortfall_v[j] = shortfall_v[j] + from_left[j].astype(F32)

                @pl.when(me < n_cube - 1)
                def _():
                    wait_right(j)
                    shortfall_v[j] = shortfall_v[j] + from_right[j].astype(F32)

                mean = shortfall_v[j] * (1.0 / n_cube)
                shortfall_v[j] = mean
                mean_out[j] = mean.astype(BF16)
                for level in range(grp_bits):
                    mean_copy(level, j).start()

    def settle(step):
        j = step - my_reach - SWAP

        @pl.when(valid(j))
        def _():
            @pl.when(me == owner(j))
            def _():
                mean = shortfall_v[j]
                combined = mean
                for level in range(grp_bits):
                    mean_copy(level, j).wait_recv()
                    combined = combined + mean_in[level, j].astype(F32)
                shortfall = combined * (1.0 / (grp_bits + 1)) - mean
                fix[j] = shortfall.astype(BF16)

                @pl.when(me > 0)
                def _():
                    fix_copy(0, j).start()

                @pl.when(me < n_cube - 1)
                def _():
                    fix_copy(1, j).start()

                spread[...] += jnp.sum((shortfall * shortfall).reshape(CHUNK // 8, 8, width), axis=0)
                finish(j, shortfall)

    def descend(step, at):
        away = jnp.where(me < at, at - me, me - at)
        j = step - reach(at) - SWAP - away * BACK

        @pl.when(jnp.logical_and(valid(j), me != at))
        def _():
            @pl.when(owner(j) == at)
            def _():
                copy(fix.at[j], fix.at[j], fix_send.at[0, j], fix_recv.at[j], cube=me).wait_recv()
                if at > 1:
                    @pl.when(jnp.logical_and(me < at, me > 0))
                    def _():
                        fix_copy(0, j).start()
                if at < n_cube - 2:
                    @pl.when(jnp.logical_and(me > at, me < n_cube - 1))
                    def _():
                        fix_copy(1, j).start()
                finish(j, fix[j].astype(F32))

    last_settle = max(chunks - 1 + reach(high), min(ENDS, chunks) - 1 + reach(0)) + SWAP
    last_step = max(
        chunks - 1 + reach(high) + high * BACK, min(ENDS, chunks) - 1 + reach(0) + (n_cube - 1) * BACK
    ) + SWAP

    def run(step, carry):
        @pl.when(step < chunks)
        def _():
            mix(step)

        climb(step)
        own(step)
        settle(step)
        @pl.when(step == last_settle)
        def _():
            spread_grp[grp] = spread[...]
            for d in range(1, n_grp):
                spread_copy_grp(d).start()

        for at in owners:
            descend(step, at)
        return carry

    lax.fori_loop(0, last_step + 1, run, 0)

    for d in range(1, n_grp):
        src = (grp + d) % n_grp
        copy(spread_grp.at[src], spread_grp.at[src], sg_send.at[d], sg_recv.at[src], grp=grp).wait_recv()
    here = jnp.sum(spread_grp[pl.ds(0, n_grp)], axis=0)
    spread_grp[n_grp] = here
    spread_cube[me] = here
    for d in range(1, n_cube):
        spread_copy_cube(d).start()

    def drain(j, carry):
        o = owner(j)

        @pl.when(me != o)
        def _():
            copy(outgoing.at[j], outgoing.at[j], up_send.at[j], left_recv.at[j], cube=me).wait_send()

        @pl.when(me == o)
        def _():
            for level in range(grp_bits):
                mean_copy(level, j).wait_send()

        @pl.when(jnp.logical_and(me <= o, me > 0))
        def _():
            fix_copy(0, j).wait_send()

        @pl.when(jnp.logical_and(me >= o, me < n_cube - 1))
        def _():
            fix_copy(1, j).wait_send()

        return carry

    lax.fori_loop(0, chunks, drain, 0)
    for d in range(1, n_grp):
        spread_copy_grp(d).wait_send()
    for d in range(1, n_cube):
        src = (me + d) % n_cube
        copy(spread_cube.at[src], spread_cube.at[src], sc_send.at[d], sc_recv.at[src], cube=me).wait_recv()
        spread_copy_cube(d).wait_send()
    whole = jnp.sum(spread_cube[...], axis=0)
    whole = jnp.sum(jnp.sum(whole, axis=0, keepdims=True), axis=1, keepdims=True)
    consensus[...] = jnp.broadcast_to(jnp.sqrt(whole / (n_grp * rows * width)), consensus.shape)


def local(params, estimate, neighbour_sum, gradient, block_ids):
    n_cube, n_grp = lax.axis_size("cube"), lax.axis_size("grp")
    rows, width = params.shape[2:]
    kept = block_ids.shape[2]
    cube_bits, grp_bits = n_cube.bit_length() - 1, n_grp.bit_length() - 1
    chunks = rows // CHUNK
    slab = jax.ShapeDtypeStruct((rows, width), F32)
    dma = pltpu.SemaphoreType.DMA
    pieces = (chunks, CHUNK, width)
    hbm = pl.BlockSpec(memory_space=pltpu.HBM)
    vmem = pl.BlockSpec(memory_space=pltpu.VMEM)
    out = pl.pallas_call(
        functools.partial(kernel, n_cube, n_grp),
        out_shape=(slab, slab, slab, jax.ShapeDtypeStruct((1, width), F32)),
        in_specs=[hbm] * 4 + [vmem],
        out_specs=(vmem,) * 4,
        scratch_shapes=[
            pltpu.VMEM((rows, width), BF16),
            pltpu.VMEM((kept, width), BF16),
            pltpu.VMEM((cube_bits * kept, width), BF16),
            pltpu.VMEM((cube_bits, 1, kept), jnp.int32),
            pltpu.VMEM(pieces, BF16),
            pltpu.VMEM(pieces, BF16),
            pltpu.VMEM(pieces, BF16),
            pltpu.VMEM(pieces, BF16),
            pltpu.VMEM((grp_bits,) + pieces, BF16),
            pltpu.VMEM(pieces, BF16),
            pltpu.VMEM(pieces, F32),
            pltpu.VMEM((8, width), F32),
            pltpu.VMEM((n_grp + 1, 8, width), F32),
            pltpu.VMEM((n_cube, 8, width), F32),
            dma((4, PIECES)),
            dma((cube_bits,)),
            dma((cube_bits,)),
            dma((cube_bits,)),
            dma((cube_bits,)),
            dma((chunks,)),
            dma((chunks,)),
            dma((chunks,)),
            dma((grp_bits, chunks)),
            dma((grp_bits, chunks)),
            dma((2, chunks)),
            dma((chunks,)),
            dma((n_grp,)),
            dma((n_grp,)),
            dma((n_cube,)),
            dma((n_cube,)),
        ],
        compiler_params=pltpu.CompilerParams(
            collective_id=0, has_side_effects=True, vmem_limit_bytes=40 * 1024 * 1024
        ),
    )(
        *(
            pltpu.with_memory_space_constraint(slab[0, 0], pltpu.HBM)
            for slab in (params, estimate, neighbour_sum, gradient)
        ),
        block_ids[0],
    )
    return (out[0][None, None], out[1][None, None], out[2][None, None], out[3][0, :1])


def solution(mesh):
    in_specs = (
        P("grp", "cube", None, None),
        P("grp", "cube", None, None),
        P("grp", "cube", None, None),
        P("grp", "cube", None, None),
        P("grp", "cube", None),
    )
    out_specs = (
        P("grp", "cube", None, None),
        P("grp", "cube", None, None),
        P("grp", "cube", None, None),
        P(),
    )
    return jax.shard_map(local, mesh=mesh, in_specs=in_specs, out_specs=out_specs, check_vma=False)
```

```python
import functools
import heapq

import jax
import jax.numpy as jnp
from jax import lax
from jax.experimental import pallas as pl
from jax.experimental.pallas import tpu as pltpu
from jax.sharding import PartitionSpec as P

LEARN_RATE = 0.1
INNER_RATE = 0.6
OUTER_RATE = 0.5
CHUNK = 128
ENDS = 16
WIRE = 0.7
DELAY = 2.0
LATE = 3.0
BLOCK = 128
PIECES = 4

MESH = pl.DeviceIdType.MESH
F32, BF16 = jnp.float32, jnp.bfloat16


def owner_of(j, n_cube):
    if j < ENDS and j % 4 >= 2:
        return (j % 2) * (n_cube - 1)
    return n_cube // 2 - 1 + j % 2


def plan(n_cube, chunks):
    work, order, busy, link = [], [[] for _ in range(n_cube)], [0.0] * n_cube, {}
    met, last = {}, [0.0] * n_cube
    count = 0

    def push(at, device, kind, j):
        nonlocal count
        heapq.heappush(work, (at, count, device, kind, j))
        count += 1

    def send(at, device, to, scale=1.0):
        key = (device, to)
        link[key] = max(at, link.get(key, 0.0)) + WIRE * scale
        return link[key] + DELAY

    for device in range(n_cube):
        for j in range(chunks):
            push(0.25 * j, device, "mix", j)
    started = [0] * n_cube

    def meet(at, device, j):
        o = owner_of(j, n_cube)
        key = (device, j)
        need = 1 + (device > 0) + (device < n_cube - 1) if device == o else 1 + (0 < device < n_cube - 1)
        seen = met.setdefault(key, [])
        seen.append(at)
        if len(seen) == need:
            push(max(seen), device, "own" if device == o else "climb", j)

    while work:
        at, _, device, kind, j = heapq.heappop(work)
        if at < busy[device]:
            push(busy[device], device, kind, j)
            continue
        order[device].append((kind, j))
        busy[device] = at + (0.25 if kind == "mix" else 0.15)
        now = busy[device]
        o = owner_of(j, n_cube)
        if kind == "mix":
            first = device in (0, n_cube - 1) and device != o
            meet(max(now, 0.9 * WIRE * started[device]) if first else now, device, j)
            started[device] += first
        elif kind == "climb":
            to = device + 1 if device < o else device - 1
            meet(send(now, device, to), to, j)
        elif kind == "own":
            late = LATE if device in (0, n_cube - 1) else 0.0
            push(send(now, device, "swap") + late, device, "settle", j)
        else:
            if kind == "settle":
                last[device] = now
            if device <= o and device > 0:
                push(send(now, device, device - 1), device - 1, "descend", j)
            if device >= o and device < n_cube - 1:
                push(send(now, device, device + 1), device + 1, "descend", j)
    return order


def kernel(
    n_cube, n_grp,
    params, estimate, neighbour_sum, gradient, ids,
    p_v, e_v, n_v, consensus,
    g_v, picked, theirs, their_ids,
    from_left, from_right, outgoing, mean_out, mean_in, fix, shortfall_v,
    spread, spread_grp, spread_cube,
    load_sem, pick_send, pick_recv, id_send, id_recv,
    up_send, left_recv, right_recv, mean_send, mean_recv,
    fix_send, fix_recv,
    sg_send, sg_recv, sc_send, sc_recv,
):
    me, grp = lax.axis_index("cube"), lax.axis_index("grp")
    rows, width = p_v.shape
    kept = picked.shape[0]
    chunks = rows // CHUNK
    cube_bits, grp_bits = n_cube.bit_length() - 1, n_grp.bit_length() - 1
    piece = rows // PIECES

    def load(which, at):
        src, dst = ((params, p_v), (gradient, g_v), (estimate, e_v), (neighbour_sum, n_v))[which]
        window = pl.ds(at * piece, piece)
        return pltpu.make_async_copy(src.at[window], dst.at[window], load_sem.at[which, at])

    barrier = pltpu.get_barrier_semaphore()
    for d in range(1, n_cube):
        pl.semaphore_signal(barrier, inc=1, device_id={"cube": (me + d) % n_cube}, device_id_type=MESH)
    for d in range(1, n_grp):
        pl.semaphore_signal(barrier, inc=1, device_id={"grp": (grp + d) % n_grp}, device_id_type=MESH)
    for at in range(PIECES):
        for which in range(3):
            load(which, at).start()
    for at in range(PIECES):
        load(3, at).start()

    def flip(index, level):
        bit = 1 << level
        return index + bit - 2 * bit * ((index // bit) % 2)

    def copy(src, dst, send, recv, **device):
        return pltpu.make_async_remote_copy(
            src_ref=src, dst_ref=dst, send_sem=send, recv_sem=recv, device_id=device, device_id_type=MESH
        )

    def id_copy(level):
        return copy(ids, their_ids.at[level], id_send.at[level], id_recv.at[level], cube=flip(me, level))

    def pick_copy(level):
        return copy(
            picked, theirs.at[pl.ds(level * kept, kept)], pick_send.at[level], pick_recv.at[level],
            cube=flip(me, level),
        )

    square = (kept, kept)
    own_ids = ids[...]
    diagonal = lax.broadcasted_iota(jnp.int32, square, 0) == lax.broadcasted_iota(jnp.int32, square, 1)
    id_column = jnp.sum(jnp.where(diagonal, jnp.broadcast_to(own_ids, square), 0), axis=1, keepdims=True)

    def pick(j, total):
        window = pl.ds(pl.multiple_of(j * CHUNK, CHUNK), CHUNK)
        stepped = p_v[window, :] - LEARN_RATE * g_v[window, :].astype(F32)
        p_v[window, :] = stepped
        change = (stepped - e_v[window, :]).astype(BF16)
        row = lax.broadcasted_iota(jnp.int32, (kept, CHUNK), 1) + j * CHUNK
        hot = (row == id_column).astype(F32).astype(BF16)
        return total + jnp.dot(hot, change, preferred_element_type=F32)

    total = jnp.zeros((kept, width), F32)
    for at in range(PIECES):
        for which in range(3):
            load(which, at).wait()
        each = piece // CHUNK
        total = lax.fori_loop(at * each, (at + 1) * each, pick, total)
    picked[...] = total.astype(BF16)
    pl.semaphore_wait(barrier, n_cube + n_grp - 2)
    for level in range(cube_bits):
        id_copy(level).start()
    for level in range(cube_bits):
        pick_copy(level).start()
    for at in range(PIECES):
        load(3, at).wait()
    spread[...] = jnp.zeros_like(spread)
    for level in range(cube_bits):
        id_copy(level).wait()
    for level in range(cube_bits):
        pick_copy(level).wait()

    def blocks(j, work):
        def one(at, carry):
            work(pl.ds(pl.multiple_of(j * CHUNK + at * BLOCK, BLOCK), BLOCK), pl.ds(pl.multiple_of(at * BLOCK, BLOCK), BLOCK))
            return carry

        lax.fori_loop(0, CHUNK // BLOCK, one, 0)

    def mix(j):
        def work(window, part):
            row = lax.broadcasted_iota(jnp.int32, (BLOCK, kept), 0) + window.start

            def hot(names):
                return (row == names).astype(F32).astype(BF16)

            e = e_v[window, :] + jnp.dot(hot(own_ids), picked[...], preferred_element_type=F32)
            marks = jnp.concatenate([hot(their_ids[level]) for level in range(cube_bits)], axis=1)
            s = n_v[window, :] + jnp.dot(marks, theirs[...], preferred_element_type=F32)
            e_v[window, :] = e
            n_v[window, :] = s
            p_v[window, :] = p_v[window, :] + (INNER_RATE / (cube_bits + 1)) * (s - cube_bits * e)

        blocks(j, work)

    across = [flip(grp, level) for level in range(grp_bits)]

    def climb_copy(role, j):
        if role < owner_of(j, n_cube):
            return copy(outgoing.at[j], from_left.at[j], up_send.at[j], left_recv.at[j], cube=role + 1)
        return copy(outgoing.at[j], from_right.at[j], up_send.at[j], right_recv.at[j], cube=role - 1)

    def wait_left(j):
        copy(from_left.at[j], from_left.at[j], up_send.at[j], left_recv.at[j], cube=me).wait_recv()

    def wait_right(j):
        copy(from_right.at[j], from_right.at[j], up_send.at[j], right_recv.at[j], cube=me).wait_recv()

    def mean_copy(level, j):
        return copy(
            mean_out.at[j], mean_in.at[level, j], mean_send.at[level, j], mean_recv.at[level, j],
            grp=across[level],
        )

    def fix_copy(side, j, to):
        return copy(fix.at[j], fix.at[j], fix_send.at[side, j], fix_recv.at[j], cube=to)

    def fix_targets(role, j):
        o = owner_of(j, n_cube)
        low = [(0, role - 1)] if role <= o and role > 0 else []
        return low + ([(1, role + 1)] if role >= o and role < n_cube - 1 else [])

    def climb(role, j):
        chain = None
        if role < owner_of(j, n_cube):
            if role > 0:
                wait_left(j)
                chain = from_left
        elif role < n_cube - 1:
            wait_right(j)
            chain = from_right

        def work(window, part):
            value = p_v[window, :]
            if chain is not None:
                value = value + chain[j, part, :].astype(F32)
            outgoing[j, part, :] = value.astype(BF16)

        blocks(j, work)
        climb_copy(role, j).start()

    def own(role, j):
        if role > 0:
            wait_left(j)
        if role < n_cube - 1:
            wait_right(j)

        def work(window, part):
            mean = p_v[window, :]
            if role > 0:
                mean = mean + from_left[j, part, :].astype(F32)
            if role < n_cube - 1:
                mean = mean + from_right[j, part, :].astype(F32)
            mean = mean * (1.0 / n_cube)
            shortfall_v[j, part, :] = mean
            mean_out[j, part, :] = mean.astype(BF16)

        blocks(j, work)
        for level in reversed(range(grp_bits)):
            mean_copy(level, j).start()

    def settle(role, j):
        for level in range(grp_bits):
            mean_copy(level, j).wait_recv()

        def work(window, part):
            mean = shortfall_v[j, part, :]
            combined = mean
            for level in range(grp_bits):
                combined = combined + mean_in[level, j, part, :].astype(F32)
            shortfall = combined * (1.0 / (grp_bits + 1)) - mean
            shortfall_v[j, part, :] = shortfall
            fix[j, part, :] = shortfall.astype(BF16)

        blocks(j, work)
        for side, to in fix_targets(role, j):
            fix_copy(side, j, to).start()

        def rest(window, part):
            shortfall = shortfall_v[j, part, :]
            spread[...] += jnp.sum((shortfall * shortfall).reshape(BLOCK // 8, 8, width), axis=0)
            p_v[window, :] = p_v[window, :] + OUTER_RATE * shortfall

        blocks(j, rest)

    def descend(role, j):
        copy(fix.at[j], fix.at[j], fix_send.at[0, j], fix_recv.at[j], cube=me).wait_recv()
        for side, to in fix_targets(role, j):
            fix_copy(side, j, to).start()

        def work(window, part):
            p_v[window, :] = p_v[window, :] + OUTER_RATE * fix[j, part, :].astype(F32)

        blocks(j, work)

    def spread_copy_grp(d):
        return copy(spread, spread_grp.at[grp], sg_send.at[d], sg_recv.at[grp], grp=(grp + d) % n_grp)

    def spread_copy_cube(d):
        return copy(
            spread_grp.at[n_grp], spread_cube.at[me], sc_send.at[d], sc_recv.at[me], cube=(me + d) % n_cube
        )

    def spread_first():
        spread_grp[grp] = spread[...]
        for d in range(1, n_grp):
            spread_copy_grp(d).start()

    def spread_second():
        for d in range(1, n_grp):
            src = (grp + d) % n_grp
            copy(spread_grp.at[src], spread_grp.at[src], sg_send.at[d], sg_recv.at[src], grp=grp).wait_recv()
        here = jnp.sum(spread_grp[pl.ds(0, n_grp)], axis=0)
        spread_grp[n_grp] = here
        spread_cube[me] = here
        for d in range(1, n_cube):
            spread_copy_cube(d).start()

    order = plan(n_cube, chunks)

    def run(role):
        steps = order[role]
        settles = [at for at, (kind, _) in enumerate(steps) if kind == "settle"]
        first = settles[-1] if settles else 0
        second = min(first + 3, len(steps) - 1)
        for at, (kind, j) in enumerate(steps):
            if kind == "mix":
                mix(j)
            else:
                {"climb": climb, "own": own, "settle": settle, "descend": descend}[kind](role, j)
            if at == first:
                spread_first()
            if at == second:
                spread_second()
        for j in range(chunks):
            if role == owner_of(j, n_cube):
                for level in range(grp_bits):
                    mean_copy(level, j).wait_send()
            else:
                climb_copy(role, j).wait_send()
            for side, to in fix_targets(role, j):
                fix_copy(side, j, to).wait_send()

    for role in range(n_cube):
        pl.when(me == role)(functools.partial(run, role))

    for d in range(1, n_grp):
        spread_copy_grp(d).wait_send()
    for d in range(1, n_cube):
        src = (me + d) % n_cube
        copy(spread_cube.at[src], spread_cube.at[src], sc_send.at[d], sc_recv.at[src], cube=me).wait_recv()
        spread_copy_cube(d).wait_send()
    whole = jnp.sum(spread_cube[...], axis=0)
    whole = jnp.sum(jnp.sum(whole, axis=0, keepdims=True), axis=1, keepdims=True)
    consensus[...] = jnp.broadcast_to(jnp.sqrt(whole / (n_grp * rows * width)), consensus.shape)


def local(params, estimate, neighbour_sum, gradient, block_ids):
    n_cube, n_grp = lax.axis_size("cube"), lax.axis_size("grp")
    rows, width = params.shape[2:]
    kept = block_ids.shape[2]
    cube_bits, grp_bits = n_cube.bit_length() - 1, n_grp.bit_length() - 1
    chunks = rows // CHUNK
    slab = jax.ShapeDtypeStruct((rows, width), F32)
    dma = pltpu.SemaphoreType.DMA
    pieces = (chunks, CHUNK, width)
    hbm = pl.BlockSpec(memory_space=pltpu.HBM)
    vmem = pl.BlockSpec(memory_space=pltpu.VMEM)
    out = pl.pallas_call(
        functools.partial(kernel, n_cube, n_grp),
        out_shape=(slab, slab, slab, jax.ShapeDtypeStruct((1, width), F32)),
        in_specs=[hbm] * 4 + [vmem],
        out_specs=(vmem,) * 4,
        scratch_shapes=[
            pltpu.VMEM((rows, width), BF16),
            pltpu.VMEM((kept, width), BF16),
            pltpu.VMEM((cube_bits * kept, width), BF16),
            pltpu.VMEM((cube_bits, 1, kept), jnp.int32),
            pltpu.VMEM(pieces, BF16),
            pltpu.VMEM(pieces, BF16),
            pltpu.VMEM(pieces, BF16),
            pltpu.VMEM(pieces, BF16),
            pltpu.VMEM((grp_bits,) + pieces, BF16),
            pltpu.VMEM(pieces, BF16),
            pltpu.VMEM(pieces, F32),
            pltpu.VMEM((8, width), F32),
            pltpu.VMEM((n_grp + 1, 8, width), F32),
            pltpu.VMEM((n_cube, 8, width), F32),
            dma((4, PIECES)),
            dma((cube_bits,)),
            dma((cube_bits,)),
            dma((cube_bits,)),
            dma((cube_bits,)),
            dma((chunks,)),
            dma((chunks,)),
            dma((chunks,)),
            dma((grp_bits, chunks)),
            dma((grp_bits, chunks)),
            dma((2, chunks)),
            dma((chunks,)),
            dma((n_grp,)),
            dma((n_grp,)),
            dma((n_cube,)),
            dma((n_cube,)),
        ],
        compiler_params=pltpu.CompilerParams(
            collective_id=0, has_side_effects=True, vmem_limit_bytes=40 * 1024 * 1024
        ),
    )(
        *(
            pltpu.with_memory_space_constraint(slab[0, 0], pltpu.HBM)
            for slab in (params, estimate, neighbour_sum, gradient)
        ),
        block_ids[0],
    )
    return (out[0][None, None], out[1][None, None], out[2][None, None], out[3][0, :1])


def solution(mesh):
    in_specs = (
        P("grp", "cube", None, None),
        P("grp", "cube", None, None),
        P("grp", "cube", None, None),
        P("grp", "cube", None, None),
        P("grp", "cube", None),
    )
    out_specs = (
        P("grp", "cube", None, None),
        P("grp", "cube", None, None),
        P("grp", "cube", None, None),
        P(),
    )
    return jax.shard_map(local, mesh=mesh, in_specs=in_specs, out_specs=out_specs, check_vma=False)
```
